32 devices in a mesh: lon: 8 (over y, x, core), lat: 4 (over z).
Axes of the slice: x: 2, y: 2, z: 4, core: 2. Of those that a mesh axis runs over, the one named last changes fastest.
Arguments:
- fields: bfloat16 [4, 128, 32, 1024], P(None, None, 'lat', 'lon'), may hold values from -12 to 12
- bracket: int32 [32, 32, 1024], P(None, 'lat', 'lon'), may hold values from 0 to 126, as said below
- fraction: bfloat16 [32, 32, 1024], P(None, 'lat', 'lon'), may hold values from 0 to 1
Outputs:
- on_pressure: bfloat16 [4, 32, 32, 1024], P(None, None, ('lat', 'lon'))
- zonal_mean: float32 [4, 32, 32], P(None, None, ('lat', 'lon'))
- meridional: float32 [4, 32, 32], P(None, None, ('lat', 'lon'))
The draws below stay inside these ranges and needn't reach their ends.
Inputs may be any that keep to these rules, and one draw needn't show every extreme that they name: bracket[p, r, c] - min(p * 4, 112) lies in 0 to 14 for every column, and each of these offsets occurs.
All inputs are finite; a program needn't handle non-finite values.
Results may differ from the reference program's by a relative error of at most 0.0012.
Values may be sent and summed in bfloat16 or wider, within the bound.
A program may use at most 128 MiB of HBM per device.

```python
import jax
import jax.numpy as jnp
from jax import lax

VARS = 4
LEV = 128
PLEV = 32
WINDOW = 16
NLAT = 32
NLON = 1024


def draw_fields(key, part):
    key_noise = jax.random.fold_in(key, 11)
    key_offset = jax.random.fold_in(key, 12)
    noise_part = jnp.clip(jax.random.normal(key_noise, (VARS, LEV, NLAT, NLON), jnp.float32), -4.0, 4.0)
    offset = jax.random.uniform(key_offset, (VARS, LEV, NLAT, 1), jnp.float32, -4.0, 4.0)
    values = noise_part + offset
    return values.astype(jnp.bfloat16)


def draw_bracket(key, part):
    key_offset = jax.random.fold_in(key, 21)
    level_step = LEV // PLEV
    pressure_index = jnp.arange(PLEV, dtype=jnp.int32).reshape(PLEV, 1, 1)
    window_base = jnp.minimum(pressure_index * level_step, LEV - WINDOW)
    offsets = jax.random.randint(key_offset, (PLEV, NLAT, NLON), 0, WINDOW - 1, dtype=jnp.int32)
    return (window_base + offsets).astype(jnp.int32)


def shard_levels(key, shape, cuts, low, largest):
    def one(dim, blocks):
        steps = jax.random.uniform(jax.random.fold_in(jax.random.fold_in(key, 6), dim), (blocks,), jnp.float32, low / len(cuts), largest / len(cuts))
        return jnp.repeat(jnp.exp(steps), shape[dim] // blocks).reshape((-1,) + (1,) * (len(shape) - dim - 1))

    level = one(*cuts[0])
    for cut in cuts[1:]:
        level = level * one(*cut)
    return level


def setup_inputs(seed: int = 0) -> dict:
    streams_of = jax.random.split(jax.random.key(seed), 4)
    return {
        "fields": draw_fields(jax.random.fold_in(streams_of[3], 71), 0),
        "bracket": draw_bracket(jax.random.fold_in(streams_of[3], 71), 0),
        "fraction": jnp.clip(1.0 * jax.random.uniform(streams_of[2], (PLEV, NLAT, NLON), jnp.float32) ** shard_levels(streams_of[2], (PLEV, NLAT, NLON), ((1, 4), (2, 8)), -0.2, 0.2), 0.0, 1.0).astype(jnp.bfloat16),
    }


def interpolate(block, bracket, fraction):
    index = jnp.broadcast_to(bracket[None], (block.shape[0],) + bracket.shape)
    lower_level = jnp.take_along_axis(block, index, axis=1).astype(jnp.float32)
    upper_level = jnp.take_along_axis(block, index + 1, axis=1).astype(jnp.float32)
    weight = fraction.astype(jnp.float32)[None]
    return (lower_level + weight * (upper_level - lower_level)).astype(jnp.bfloat16)


def reference(fields, bracket, fraction):
    on_pressure = lax.map(lambda single: interpolate(single[None], bracket, fraction)[0], fields)
    zonal_mean = jnp.sum(on_pressure.astype(jnp.float32), axis=3) / jnp.float32(NLON)
    centered = 0.5 * (zonal_mean[:, :, 2:] - zonal_mean[:, :, :-2])
    first_row = zonal_mean[:, :, 1:2] - zonal_mean[:, :, 0:1]
    last_row = zonal_mean[:, :, -1:] - zonal_mean[:, :, -2:-1]
    meridional = jnp.concatenate([first_row, centered, last_row], axis=2)
    return on_pressure, zonal_mean, meridional
```

```python
import functools

import jax
import jax.numpy as jnp
from jax import lax
from jax.experimental import pallas as pl
from jax.experimental.pallas import tpu as pltpu
from jax.sharding import PartitionSpec as P

WINDOW = 16
TILE = 8
MESH = pl.DeviceIdType.MESH


def select_pair(levels, masks):
    bit = len(levels) // 2
    for mask in masks:
        levels = [
            jnp.where(mask, levels[k + bit], levels[k]) if k + bit < len(levels) else levels[k]
            for k in range(bit + 1)
        ]
        bit //= 2
    return levels


def kernel(
    lon_count, lat_count, fields_hbm, bracket_hbm, fraction_hbm,
    out_ref, zonal_ref, merid_ref,
    fields, bracket, fraction, send, sums, cross_lo, cross_hi,
    in_sem, field_sem, own_sem, send_sem, recv_sem, sum_send, sum_recv,
    cross_send, lo_recv, hi_recv,
):
    var_count, level_count, row_count, lons = fields.shape
    plev_count = bracket.shape[0]
    own = row_count // lon_count
    group_size = min(TILE, plev_count)
    level_step = level_count // plev_count
    me = lax.axis_index("lon")
    band = lax.axis_index("lat")
    next_band = (band + 1) % lat_count
    prev_band = (band + lat_count - 1) % lat_count
    has_lo = jnp.logical_and(me == 0, band > 0)
    has_hi = jnp.logical_and(me == lon_count - 1, band < lat_count - 1)
    my_lons = pl.ds(pl.multiple_of(me * lons, 128), lons)

    get_bracket = pltpu.make_async_copy(bracket_hbm, bracket, in_sem.at[0])
    get_fraction = pltpu.make_async_copy(fraction_hbm, fraction, in_sem.at[1])

    def get_fields(v):
        return pltpu.make_async_copy(fields_hbm.at[v], fields.at[v], field_sem.at[v])

    get_bracket.start()
    get_fraction.start()
    for v in range(var_count):
        get_fields(v).start()

    barrier = pltpu.get_barrier_semaphore()
    for step in range(1, lon_count):
        peer = (me + step) % lon_count
        pl.semaphore_signal(barrier, inc=1, device_id={"lon": peer}, device_id_type=MESH)

    @pl.when(has_lo)
    def _():
        for l in range(lon_count):
            pl.semaphore_signal(barrier, inc=1, device_id={"lon": l, "lat": prev_band}, device_id_type=MESH)

    @pl.when(has_hi)
    def _():
        for l in range(lon_count):
            pl.semaphore_signal(barrier, inc=1, device_id={"lon": l, "lat": next_band}, device_id_type=MESH)

    def block_copy(v, step):
        peer = (me + step) % lon_count
        return pltpu.make_async_remote_copy(
            src_ref=send.at[v, pl.ds(peer * own, own)],
            dst_ref=out_ref.at[v, :, :, my_lons],
            send_sem=send_sem.at[step],
            recv_sem=recv_sem.at[step],
            device_id={"lon": peer},
            device_id_type=MESH,
        )

    def own_copy(v):
        return pltpu.make_async_copy(
            send.at[v, pl.ds(me * own, own)], out_ref.at[v, :, :, my_lons], own_sem.at[v]
        )

    def sum_copy(step):
        return pltpu.make_async_remote_copy(
            src_ref=sums.at[me],
            dst_ref=sums.at[me],
            send_sem=sum_send.at[step],
            recv_sem=sum_recv.at[step],
            device_id={"lon": (me + step) % lon_count},
            device_id_type=MESH,
        )

    def up_copy():
        return pltpu.make_async_remote_copy(
            src_ref=sums.at[me], dst_ref=cross_lo.at[me],
            send_sem=cross_send.at[0], recv_sem=lo_recv.at[me],
            device_id={"lon": 0, "lat": next_band}, device_id_type=MESH,
        )

    def down_copy():
        return pltpu.make_async_remote_copy(
            src_ref=sums.at[me], dst_ref=cross_hi.at[me],
            send_sem=cross_send.at[1], recv_sem=hi_recv.at[me],
            device_id={"lon": lon_count - 1, "lat": prev_band}, device_id_type=MESH,
        )

    get_bracket.wait()
    get_fraction.wait()
    ones = jnp.ones((TILE, lons), jnp.bfloat16)

    @pl.loop(0, var_count)
    def _(v):
        get_fields(v).wait()

        @pl.loop(0, row_count // TILE)
        def _(tile):
            rows = pl.ds(pl.multiple_of(tile * TILE, TILE), TILE)
            loaded, group = {}, []
            for p in range(plev_count):
                base = min(p * level_step, level_count - WINDOW)
                for k in range(base, base + WINDOW):
                    if k not in loaded:
                        loaded[k] = fields[v, k, rows, :].astype(jnp.float32)
                offset = bracket[p, rows, :] - base
                masks, bit = [], WINDOW // 2
                while bit:
                    masks.append((offset & bit) != 0)
                    bit //= 2
                lower, upper = select_pair([loaded[base + k] for k in range(WINDOW)], masks)
                weight = fraction[p, rows, :].astype(jnp.float32)
                group.append(lower + weight * (upper - lower))
                if len(group) == group_size:
                    by_row = jnp.transpose(jnp.stack(group), (1, 0, 2)).astype(jnp.bfloat16)
                    send[v, rows, p + 1 - group_size : p + 1, :] = by_row
                    group = []
            rounded = send[v, rows].reshape(TILE * plev_count, lons)
            total = lax.dot_general(
                ones, rounded, (((1,), (1,)), ((), ())), preferred_element_type=jnp.float32
            )
            width = TILE * plev_count
            sums[me, v, :, pl.ds(pl.multiple_of(tile * width, width), width)] = total[0:1]

        @pl.when(v == 0)
        def _():
            beyond = (band < lat_count - 1).astype(jnp.int32) + (band > 0).astype(jnp.int32)
            pl.semaphore_wait(barrier, lon_count - 1 + beyond)

        for step in range(lon_count - 1, 0, -1):
            block_copy(v, step).start()
        own_copy(v).start()

    @pl.when(band < lat_count - 1)
    def _():
        up_copy().start()

    @pl.when(band > 0)
    def _():
        down_copy().start()

    for step in range(1, lon_count):
        sum_copy(step).start()

    for step in range(1, lon_count):
        sum_copy(step).wait_recv()
    mean = sums[0]
    for l in range(1, lon_count):
        mean = mean + sums[l]
    count = jnp.float32(lons * lon_count)
    mean = mean / count
    width = row_count * plev_count

    def row_of(q):
        shift = (2 * width - q * plev_count) % width
        return pltpu.roll(mean.reshape(var_count, width), shift, 1)[:, :plev_count]

    def edge(cross, recv, row):
        for l in range(lon_count):
            pltpu.make_async_copy(cross.at[l], cross.at[l], recv.at[l]).wait()
        total = cross[0]
        for l in range(1, lon_count):
            total = total + cross[l]
        total = (total / count).reshape(var_count, width)
        return total[:, row * plev_count : (row + 1) * plev_count]

    first = me * own
    for j in range(own):
        here = row_of(first + j)
        below = row_of(first + j - 1)
        above = row_of(first + j + 1)
        zonal_ref[:, j, :] = here
        lower_edge = jnp.logical_and(first + j == 0, band == 0)
        upper_edge = jnp.logical_and(first + j == row_count - 1, band == lat_count - 1)
        below = jnp.where(lower_edge, here, below)
        above = jnp.where(upper_edge, here, above)
        scale = jnp.where(jnp.logical_or(lower_edge, upper_edge), 1.0, 0.5)
        merid_ref[:, j, :] = scale * (above - below)

    @pl.when(has_lo)
    def _():
        below = edge(cross_lo, lo_recv, row_count - 1)
        above = row_of(jnp.int32(1))
        merid_ref[:, 0, :] = 0.5 * (above - below)

    @pl.when(has_hi)
    def _():
        above = edge(cross_hi, hi_recv, 0)
        below = row_of(jnp.int32(row_count - 2))
        merid_ref[:, own - 1, :] = 0.5 * (above - below)

    for v in range(var_count):
        own_copy(v).wait()
    for step in range(1, lon_count):
        source = (me + lon_count - step) % lon_count
        landed = out_ref.at[:, :, :, pl.ds(pl.multiple_of(source * lons, 128), lons)]
        pltpu.make_async_copy(landed, landed, recv_sem.at[step]).wait()
    for step in range(1, lon_count):
        peer = (me + step) % lon_count
        left = send.at[:, pl.ds(peer * own, own)]
        pltpu.make_async_copy(left, left, send_sem.at[step]).wait()
        sum_copy(step).wait_send()

    @pl.when(band < lat_count - 1)
    def _():
        up_copy().wait_send()

    @pl.when(band > 0)
    def _():
        down_copy().wait_send()


def shards(lon_count, lat_count, fields, bracket, fraction):
    var_count, level_count, row_count, lons = fields.shape
    plev_count = bracket.shape[0]
    own = row_count // lon_count
    sum_shape = (lon_count, var_count, 1, row_count * plev_count)
    dma = pltpu.SemaphoreType.DMA
    anywhere = pl.BlockSpec(memory_space=pl.ANY)
    in_vmem = pl.BlockSpec(memory_space=pltpu.VMEM)
    on_pressure, zonal_mean, meridional = pl.pallas_call(
        functools.partial(kernel, lon_count, lat_count),
        out_shape=(
            jax.ShapeDtypeStruct((var_count, own, plev_count, lons * lon_count), jnp.bfloat16),
            jax.ShapeDtypeStruct((var_count, own, plev_count), jnp.float32),
            jax.ShapeDtypeStruct((var_count, own, plev_count), jnp.float32),
        ),
        in_specs=[anywhere] * 3,
        out_specs=(anywhere, in_vmem, in_vmem),
        scratch_shapes=[
            pltpu.VMEM(fields.shape, fields.dtype),
            pltpu.VMEM(bracket.shape, bracket.dtype),
            pltpu.VMEM(fraction.shape, fraction.dtype),
            pltpu.VMEM((var_count, row_count, plev_count, lons), jnp.bfloat16),
            pltpu.VMEM(sum_shape, jnp.float32),
            pltpu.VMEM(sum_shape, jnp.float32),
            pltpu.VMEM(sum_shape, jnp.float32),
            dma((2,)),
            dma((var_count,)),
            dma((var_count,)),
            dma((lon_count,)),
            dma((lon_count,)),
            dma((lon_count,)),
            dma((lon_count,)),
            dma((2,)),
            dma((lon_count,)),
            dma((lon_count,)),
        ],
        compiler_params=pltpu.CompilerParams(
            collective_id=0, has_side_effects=True, vmem_limit_bytes=60 * 1024 * 1024
        ),
    )(fields, bracket, fraction)
    return (
        on_pressure.transpose(0, 2, 1, 3),
        zonal_mean.transpose(0, 2, 1),
        meridional.transpose(0, 2, 1),
    )


def solution(mesh):
    return jax.shard_map(
        functools.partial(shards, mesh.shape["lon"], mesh.shape["lat"]),
        mesh=mesh,
        in_specs=(P(None, None, "lat", "lon"), P(None, "lat", "lon"), P(None, "lat", "lon")),
        out_specs=(
            P(None, None, ("lat", "lon"), None),
            P(None, None, ("lat", "lon")),
            P(None, None, ("lat", "lon")),
        ),
        check_vma=False,
    )
```

```python
import functools

import jax
import jax.numpy as jnp
from jax import lax
from jax.experimental import pallas as pl
from jax.experimental.pallas import tpu as pltpu
from jax.sharding import PartitionSpec as P

WINDOW = 16
TILE = 8
MESH = pl.DeviceIdType.MESH


def select_pair(levels, masks):
    bit = len(levels) // 2
    for mask in masks:
        levels = [
            jnp.where(mask, levels[k + bit], levels[k]) if k + bit < len(levels) else levels[k]
            for k in range(bit + 1)
        ]
        bit //= 2
    return levels


def exchange(
    lon_count, lat_count, fields_hbm, bracket_hbm, fraction_hbm,
    out_ref, sums, cross_lo, cross_hi,
    fields, bracket, fraction, send,
    in_sem, field_sem, own_sem, send_sem, recv_sem, sum_send, sum_recv,
    cross_send, lo_recv, hi_recv,
):
    var_count, level_count, row_count, lons = fields.shape
    plev_count = bracket.shape[0]
    own = row_count // lon_count
    group_size = min(TILE, plev_count)
    level_step = level_count // plev_count
    me = lax.axis_index("lon")
    band = lax.axis_index("lat")
    next_band = (band + 1) % lat_count
    prev_band = (band + lat_count - 1) % lat_count
    has_lo = jnp.logical_and(me == 0, band > 0)
    has_hi = jnp.logical_and(me == lon_count - 1, band < lat_count - 1)
    my_lons = pl.ds(pl.multiple_of(me * lons, 128), lons)

    get_bracket = pltpu.make_async_copy(bracket_hbm, bracket, in_sem.at[0])
    get_fraction = pltpu.make_async_copy(fraction_hbm, fraction, in_sem.at[1])

    def get_fields(v):
        return pltpu.make_async_copy(fields_hbm.at[v], fields.at[v], field_sem.at[v])

    get_bracket.start()
    get_fraction.start()
    for v in range(var_count):
        get_fields(v).start()

    barrier = pltpu.get_barrier_semaphore()
    for step in range(1, lon_count):
        peer = (me + step) % lon_count
        pl.semaphore_signal(barrier, inc=1, device_id={"lon": peer}, device_id_type=MESH)

    @pl.when(has_lo)
    def _():
        for l in range(lon_count):
            pl.semaphore_signal(barrier, inc=1, device_id={"lon": l, "lat": prev_band}, device_id_type=MESH)

    @pl.when(has_hi)
    def _():
        for l in range(lon_count):
            pl.semaphore_signal(barrier, inc=1, device_id={"lon": l, "lat": next_band}, device_id_type=MESH)

    def block_copy(v, step):
        peer = (me + step) % lon_count
        return pltpu.make_async_remote_copy(
            src_ref=send.at[v, pl.ds(peer * own, own)],
            dst_ref=out_ref.at[v, :, :, my_lons],
            send_sem=send_sem.at[step],
            recv_sem=recv_sem.at[step],
            device_id={"lon": peer},
            device_id_type=MESH,
        )

    def own_copy(v):
        return pltpu.make_async_copy(
            send.at[v, pl.ds(me * own, own)], out_ref.at[v, :, :, my_lons], own_sem.at[v]
        )

    def sum_copy(step):
        return pltpu.make_async_remote_copy(
            src_ref=sums.at[me],
            dst_ref=sums.at[me],
            send_sem=sum_send.at[step],
            recv_sem=sum_recv.at[step],
            device_id={"lon": (me + step) % lon_count},
            device_id_type=MESH,
        )

    def up_copy():
        return pltpu.make_async_remote_copy(
            src_ref=sums.at[me], dst_ref=cross_lo.at[me],
            send_sem=cross_send.at[0], recv_sem=lo_recv.at[me],
            device_id={"lon": 0, "lat": next_band}, device_id_type=MESH,
        )

    def down_copy():
        return pltpu.make_async_remote_copy(
            src_ref=sums.at[me], dst_ref=cross_hi.at[me],
            send_sem=cross_send.at[1], recv_sem=hi_recv.at[me],
            device_id={"lon": lon_count - 1, "lat": prev_band}, device_id_type=MESH,
        )

    get_bracket.wait()
    get_fraction.wait()
    ones = jnp.ones((TILE, lons), jnp.bfloat16)

    @pl.loop(0, var_count)
    def _(v):
        get_fields(v).wait()

        @pl.loop(0, row_count // TILE)
        def _(tile):
            rows = pl.ds(pl.multiple_of(tile * TILE, TILE), TILE)
            loaded, group = {}, []
            for p in range(plev_count):
                base = min(p * level_step, level_count - WINDOW)
                for k in range(base, base + WINDOW):
                    if k not in loaded:
                        loaded[k] = fields[v, k, rows, :].astype(jnp.float32)
                offset = bracket[p, rows, :] - base
                masks, bit = [], WINDOW // 2
                while bit:
                    masks.append((offset & bit) != 0)
                    bit //= 2
                lower, upper = select_pair([loaded[base + k] for k in range(WINDOW)], masks)
                weight = fraction[p, rows, :].astype(jnp.float32)
                group.append(lower + weight * (upper - lower))
                if len(group) == group_size:
                    by_row = jnp.transpose(jnp.stack(group), (1, 0, 2)).astype(jnp.bfloat16)
                    send[v, rows, p + 1 - group_size : p + 1, :] = by_row
                    group = []
            rounded = send[v, rows].reshape(TILE * plev_count, lons)
            total = lax.dot_general(
                ones, rounded, (((1,), (1,)), ((), ())), preferred_element_type=jnp.float32
            )
            width = TILE * plev_count
            sums[me, v, :, pl.ds(pl.multiple_of(tile * width, width), width)] = total[0:1]

        @pl.when(v == 0)
        def _():
            beyond = (band < lat_count - 1).astype(jnp.int32) + (band > 0).astype(jnp.int32)
            pl.semaphore_wait(barrier, lon_count - 1 + beyond)

        for step in range(lon_count - 1, 0, -1):
            block_copy(v, step).start()
        own_copy(v).start()

    @pl.when(band < lat_count - 1)
    def _():
        up_copy().start()

    @pl.when(band > 0)
    def _():
        down_copy().start()

    for step in range(1, lon_count):
        sum_copy(step).start()

    for step in range(1, lon_count):
        sum_copy(step).wait_recv()

    @pl.when(has_lo)
    def _():
        for l in range(lon_count):
            pltpu.make_async_copy(cross_lo.at[l], cross_lo.at[l], lo_recv.at[l]).wait()

    @pl.when(has_hi)
    def _():
        for l in range(lon_count):
            pltpu.make_async_copy(cross_hi.at[l], cross_hi.at[l], hi_recv.at[l]).wait()

    for v in range(var_count):
        own_copy(v).wait()
    for step in range(1, lon_count):
        source = (me + lon_count - step) % lon_count
        landed = out_ref.at[:, :, :, pl.ds(pl.multiple_of(source * lons, 128), lons)]
        pltpu.make_async_copy(landed, landed, recv_sem.at[step]).wait()
    for step in range(1, lon_count):
        peer = (me + step) % lon_count
        left = send.at[:, pl.ds(peer * own, own)]
        pltpu.make_async_copy(left, left, send_sem.at[step]).wait()
        sum_copy(step).wait_send()

    @pl.when(band < lat_count - 1)
    def _():
        up_copy().wait_send()

    @pl.when(band > 0)
    def _():
        down_copy().wait_send()


def finish(
    lon_count, lat_count, count, rows_vmem, sums, cross_lo, cross_hi,
    out_hbm, zonal_hbm, merid_hbm, zonal, merid, sem,
):
    var_count, own, plev_count = zonal.shape
    row_count = own * lon_count
    me = lax.axis_index("lon")
    band = lax.axis_index("lat")
    has_lo = jnp.logical_and(me == 0, band > 0)
    has_hi = jnp.logical_and(me == lon_count - 1, band < lat_count - 1)
    put_rows = pltpu.make_async_copy(rows_vmem, out_hbm, sem.at[0])
    put_rows.start()

    mean = sums[0]
    for l in range(1, lon_count):
        mean = mean + sums[l]
    mean = mean / count
    width = row_count * plev_count

    def row_of(q):
        shift = (2 * width - q * plev_count) % width
        return pltpu.roll(mean.reshape(var_count, width), shift, 1)[:, :plev_count]

    def edge(cross, row):
        total = cross[0]
        for l in range(1, lon_count):
            total = total + cross[l]
        total = (total / count).reshape(var_count, width)
        return total[:, row * plev_count : (row + 1) * plev_count]

    first = me * own
    for j in range(own):
        here = row_of(first + j)
        below = row_of(first + j - 1)
        above = row_of(first + j + 1)
        zonal[:, j, :] = here
        lower_edge = jnp.logical_and(first + j == 0, band == 0)
        upper_edge = jnp.logical_and(first + j == row_count - 1, band == lat_count - 1)
        below = jnp.where(lower_edge, here, below)
        above = jnp.where(upper_edge, here, above)
        scale = jnp.where(jnp.logical_or(lower_edge, upper_edge), 1.0, 0.5)
        merid[:, j, :] = scale * (above - below)

    @pl.when(has_lo)
    def _():
        below = edge(cross_lo, row_count - 1)
        above = row_of(jnp.int32(1))
        merid[:, 0, :] = 0.5 * (above - below)

    @pl.when(has_hi)
    def _():
        above = edge(cross_hi, 0)
        below = row_of(jnp.int32(row_count - 2))
        merid[:, own - 1, :] = 0.5 * (above - below)

    put_zonal = pltpu.make_async_copy(zonal, zonal_hbm, sem.at[1])
    put_merid = pltpu.make_async_copy(merid, merid_hbm, sem.at[2])
    put_zonal.start()
    put_merid.start()
    put_rows.wait()
    put_zonal.wait()
    put_merid.wait()


def shards(lon_count, lat_count, fields, bracket, fraction):
    var_count, level_count, row_count, lons = fields.shape
    plev_count = bracket.shape[0]
    own = row_count // lon_count
    sum_shape = (lon_count, var_count, 1, row_count * plev_count)
    dma = pltpu.SemaphoreType.DMA
    anywhere = pl.BlockSpec(memory_space=pl.ANY)
    room = 2 * fields.size + 4 * bracket.size + 2 * fraction.size * (1 + var_count)
    in_vmem = pl.BlockSpec(memory_space=pltpu.VMEM)
    rows_shape = (var_count, own, plev_count, lons * lon_count)
    inputs = [pltpu.with_memory_space_constraint(x, pltpu.HBM) for x in (fields, bracket, fraction)]
    held = pl.pallas_call(
        functools.partial(exchange, lon_count, lat_count),
        out_shape=(
            pltpu.VMEM(rows_shape, jnp.bfloat16),
            pltpu.VMEM(sum_shape, jnp.float32),
            pltpu.VMEM(sum_shape, jnp.float32),
            pltpu.VMEM(sum_shape, jnp.float32),
        ),
        in_specs=[anywhere] * 3,
        out_specs=(in_vmem,) * 4,
        scratch_shapes=[
            pltpu.VMEM(fields.shape, fields.dtype),
            pltpu.VMEM(bracket.shape, bracket.dtype),
            pltpu.VMEM(fraction.shape, fraction.dtype),
            pltpu.VMEM((var_count, row_count, plev_count, lons), jnp.bfloat16),
            dma((2,)),
            dma((var_count,)),
            dma((var_count,)),
            dma((lon_count,)),
            dma((lon_count,)),
            dma((lon_count,)),
            dma((lon_count,)),
            dma((2,)),
            dma((lon_count,)),
            dma((lon_count,)),
        ],
        compiler_params=pltpu.CompilerParams(
            collective_id=0, has_side_effects=True, vmem_limit_bytes=room + (8 << 20)
        ),
    )(*inputs)
    held = [pltpu.with_memory_space_constraint(x, pltpu.VMEM) for x in held]
    mean_shape = (var_count, own, plev_count)
    on_pressure, zonal_mean, meridional = pl.pallas_call(
        functools.partial(finish, lon_count, lat_count, float(lons * lon_count)),
        out_shape=(
            jax.ShapeDtypeStruct(rows_shape, jnp.bfloat16),
            jax.ShapeDtypeStruct(mean_shape, jnp.float32),
            jax.ShapeDtypeStruct(mean_shape, jnp.float32),
        ),
        in_specs=[in_vmem] * 4,
        out_specs=(anywhere,) * 3,
        scratch_shapes=[
            pltpu.VMEM(mean_shape, jnp.float32),
            pltpu.VMEM(mean_shape, jnp.float32),
            dma((3,)),
        ],
        compiler_params=pltpu.CompilerParams(vmem_limit_bytes=8 << 20),
    )(*held)
    return (
        on_pressure.transpose(0, 2, 1, 3),
        zonal_mean.transpose(0, 2, 1),
        meridional.transpose(0, 2, 1),
    )


def solution(mesh):
    return jax.shard_map(
        functools.partial(shards, mesh.shape["lon"], mesh.shape["lat"]),
        mesh=mesh,
        in_specs=(P(None, None, "lat", "lon"), P(None, "lat", "lon"), P(None, "lat", "lon")),
        out_specs=(
            P(None, None, ("lat", "lon"), None),
            P(None, None, ("lat", "lon")),
            P(None, None, ("lat", "lon")),
        ),
        check_vma=False,
    )
```

```python
import functools

import jax
import jax.numpy as jnp
from jax import lax
from jax.experimental import pallas as pl
from jax.experimental.pallas import tpu as pltpu
from jax.sharding import PartitionSpec as P

WINDOW = 16
TILE = 8
MESH = pl.DeviceIdType.MESH


def select_pair(levels, masks):
    bit = len(levels) // 2
    for mask in masks:
        levels = [
            jnp.where(mask, levels[k + bit], levels[k]) if k + bit < len(levels) else levels[k]
            for k in range(bit + 1)
        ]
        bit //= 2
    return levels


def exchange(
    lon_count, lat_count, fields_hbm, bracket_hbm, fraction_hbm,
    out_ref, sums, cross_lo, cross_hi,
    fields, bracket, fraction, send,
    in_sem, field_sem, own_sem, send_sem, recv_sem, sum_send, sum_recv,
    cross_send, lo_recv, hi_recv,
):
    var_count, level_count, row_count, lons = fields.shape
    plev_count = bracket.shape[0]
    own = row_count // lon_count
    group_size = min(TILE, plev_count)
    level_step = level_count // plev_count
    me = lax.axis_index("lon")
    band = lax.axis_index("lat")
    next_band = (band + 1) % lat_count
    prev_band = (band + lat_count - 1) % lat_count
    has_lo = jnp.logical_and(me == 0, band > 0)
    has_hi = jnp.logical_and(me == lon_count - 1, band < lat_count - 1)
    my_lons = pl.ds(pl.multiple_of(me * lons, 128), lons)

    get_bracket = pltpu.make_async_copy(bracket_hbm, bracket, in_sem.at[0])
    get_fraction = pltpu.make_async_copy(fraction_hbm, fraction, in_sem.at[1])

    def get_fields(v):
        return pltpu.make_async_copy(fields_hbm.at[v], fields.at[v], field_sem.at[v])

    get_bracket.start()
    get_fraction.start()
    for v in range(var_count):
        get_fields(v).start()

    barrier = pltpu.get_barrier_semaphore()
    for step in range(1, lon_count):
        peer = (me + step) % lon_count
        pl.semaphore_signal(barrier, inc=1, device_id={"lon": peer}, device_id_type=MESH)

    @pl.when(has_lo)
    def _():
        for l in range(lon_count):
            pl.semaphore_signal(barrier, inc=1, device_id={"lon": l, "lat": prev_band}, device_id_type=MESH)

    @pl.when(has_hi)
    def _():
        for l in range(lon_count):
            pl.semaphore_signal(barrier, inc=1, device_id={"lon": l, "lat": next_band}, device_id_type=MESH)

    def block_copy(v, step):
        peer = (me + step) % lon_count
        return pltpu.make_async_remote_copy(
            src_ref=send.at[v, pl.ds(peer * own, own)],
            dst_ref=out_ref.at[v, :, :, my_lons],
            send_sem=send_sem.at[step],
            recv_sem=recv_sem.at[step],
            device_id={"lon": peer},
            device_id_type=MESH,
        )

    def own_copy(v):
        return pltpu.make_async_copy(
            send.at[v, pl.ds(me * own, own)], out_ref.at[v, :, :, my_lons], own_sem.at[v]
        )

    def sum_copy(step):
        return pltpu.make_async_remote_copy(
            src_ref=sums.at[me],
            dst_ref=sums.at[me],
            send_sem=sum_send.at[step],
            recv_sem=sum_recv.at[step],
            device_id={"lon": (me + step) % lon_count},
            device_id_type=MESH,
        )

    def up_copy():
        return pltpu.make_async_remote_copy(
            src_ref=sums.at[me], dst_ref=cross_lo.at[me],
            send_sem=cross_send.at[0], recv_sem=lo_recv.at[me],
            device_id={"lon": 0, "lat": next_band}, device_id_type=MESH,
        )

    def down_copy():
        return pltpu.make_async_remote_copy(
            src_ref=sums.at[me], dst_ref=cross_hi.at[me],
            send_sem=cross_send.at[1], recv_sem=hi_recv.at[me],
            device_id={"lon": lon_count - 1, "lat": prev_band}, device_id_type=MESH,
        )

    get_bracket.wait()
    get_fraction.wait()
    ones = jnp.ones((TILE, lons), jnp.bfloat16)

    @pl.loop(0, var_count)
    def _(v):
        get_fields(v).wait()

        @pl.loop(0, row_count // TILE)
        def _(tile):
            rows = pl.ds(pl.multiple_of(tile * TILE, TILE), TILE)
            loaded, group = {}, []
            for p in range(plev_count):
                base = min(p * level_step, level_count - WINDOW)
                for k in range(base, base + WINDOW):
                    if k not in loaded:
                        loaded[k] = fields[v, k, rows, :].astype(jnp.float32)
                offset = bracket[p, rows, :] - base
                masks, bit = [], WINDOW // 2
                while bit:
                    masks.append((offset & bit) != 0)
                    bit //= 2
                lower, upper = select_pair([loaded[base + k] for k in range(WINDOW)], masks)
                weight = fraction[p, rows, :].astype(jnp.float32)
                group.append(lower + weight * (upper - lower))
                if len(group) == group_size:
                    by_row = jnp.transpose(jnp.stack(group), (1, 0, 2)).astype(jnp.bfloat16)
                    send[v, rows, p + 1 - group_size : p + 1, :] = by_row
                    group = []
            rounded = send[v, rows].reshape(TILE * plev_count, lons)
            total = lax.dot_general(
                ones, rounded, (((1,), (1,)), ((), ())), preferred_element_type=jnp.float32
            )
            width = TILE * plev_count
            sums[me, v, :, pl.ds(pl.multiple_of(tile * width, width), width)] = total[0:1]

        @pl.when(v == 0)
        def _():
            beyond = (band < lat_count - 1).astype(jnp.int32) + (band > 0).astype(jnp.int32)
            pl.semaphore_wait(barrier, lon_count - 1 + beyond)

        @pl.when(v == var_count - 1)
        def _():
            @pl.when(band < lat_count - 1)
            def _():
                up_copy().start()

            @pl.when(band > 0)
            def _():
                down_copy().start()

            for step in range(1, lon_count):
                sum_copy(step).start()

        for step in range(lon_count - 1, 0, -1):
            block_copy(v, step).start()
        own_copy(v).start()

    for step in range(1, lon_count):
        sum_copy(step).wait_recv()

    @pl.when(has_lo)
    def _():
        for l in range(lon_count):
            pltpu.make_async_copy(cross_lo.at[l], cross_lo.at[l], lo_recv.at[l]).wait()

    @pl.when(has_hi)
    def _():
        for l in range(lon_count):
            pltpu.make_async_copy(cross_hi.at[l], cross_hi.at[l], hi_recv.at[l]).wait()

    for v in range(var_count):
        own_copy(v).wait()
    for step in range(1, lon_count):
        source = (me + lon_count - step) % lon_count
        landed = out_ref.at[:, :, :, pl.ds(pl.multiple_of(source * lons, 128), lons)]
        pltpu.make_async_copy(landed, landed, recv_sem.at[step]).wait()
    for step in range(1, lon_count):
        peer = (me + step) % lon_count
        left = send.at[:, pl.ds(peer * own, own)]
        pltpu.make_async_copy(left, left, send_sem.at[step]).wait()
        sum_copy(step).wait_send()

    @pl.when(band < lat_count - 1)
    def _():
        up_copy().wait_send()

    @pl.when(band > 0)
    def _():
        down_copy().wait_send()


def finish(
    lon_count, lat_count, count, rows_vmem, sums, cross_lo, cross_hi,
    out_hbm, zonal_hbm, merid_hbm, zonal, merid, sem,
):
    var_count, own, plev_count = zonal.shape
    row_count = own * lon_count
    me = lax.axis_index("lon")
    band = lax.axis_index("lat")
    has_lo = jnp.logical_and(me == 0, band > 0)
    has_hi = jnp.logical_and(me == lon_count - 1, band < lat_count - 1)
    put_rows = pltpu.make_async_copy(rows_vmem, out_hbm, sem.at[0])
    put_rows.start()

    mean = sums[0]
    for l in range(1, lon_count):
        mean = mean + sums[l]
    mean = mean / count
    width = row_count * plev_count

    def row_of(q):
        shift = (2 * width - q * plev_count) % width
        return pltpu.roll(mean.reshape(var_count, width), shift, 1)[:, :plev_count]

    def edge(cross, row):
        total = cross[0]
        for l in range(1, lon_count):
            total = total + cross[l]
        total = (total / count).reshape(var_count, width)
        return total[:, row * plev_count : (row + 1) * plev_count]

    first = me * own
    for j in range(own):
        here = row_of(first + j)
        below = row_of(first + j - 1)
        above = row_of(first + j + 1)
        zonal[:, j, :] = here
        lower_edge = jnp.logical_and(first + j == 0, band == 0)
        upper_edge = jnp.logical_and(first + j == row_count - 1, band == lat_count - 1)
        below = jnp.where(lower_edge, here, below)
        above = jnp.where(upper_edge, here, above)
        scale = jnp.where(jnp.logical_or(lower_edge, upper_edge), 1.0, 0.5)
        merid[:, j, :] = scale * (above - below)

    @pl.when(has_lo)
    def _():
        below = edge(cross_lo, row_count - 1)
        above = row_of(jnp.int32(1))
        merid[:, 0, :] = 0.5 * (above - below)

    @pl.when(has_hi)
    def _():
        above = edge(cross_hi, 0)
        below = row_of(jnp.int32(row_count - 2))
        merid[:, own - 1, :] = 0.5 * (above - below)

    put_zonal = pltpu.make_async_copy(zonal, zonal_hbm, sem.at[1])
    put_merid = pltpu.make_async_copy(merid, merid_hbm, sem.at[2])
    put_zonal.start()
    put_merid.start()
    put_rows.wait()
    put_zonal.wait()
    put_merid.wait()


def shards(lon_count, lat_count, fields, bracket, fraction):
    var_count, level_count, row_count, lons = fields.shape
    plev_count = bracket.shape[0]
    own = row_count // lon_count
    sum_shape = (lon_count, var_count, 1, row_count * plev_count)
    dma = pltpu.SemaphoreType.DMA
    anywhere = pl.BlockSpec(memory_space=pl.ANY)
    room = 2 * fields.size + 4 * bracket.size + 2 * fraction.size * (1 + var_count)
    in_vmem = pl.BlockSpec(memory_space=pltpu.VMEM)
    rows_shape = (var_count, own, plev_count, lons * lon_count)
    inputs = [pltpu.with_memory_space_constraint(x, pltpu.HBM) for x in (fields, bracket, fraction)]
    held = pl.pallas_call(
        functools.partial(exchange, lon_count, lat_count),
        out_shape=(
            pltpu.VMEM(rows_shape, jnp.bfloat16),
            pltpu.VMEM(sum_shape, jnp.float32),
            pltpu.VMEM(sum_shape, jnp.float32),
            pltpu.VMEM(sum_shape, jnp.float32),
        ),
        in_specs=[anywhere] * 3,
        out_specs=(in_vmem,) * 4,
        scratch_shapes=[
            pltpu.VMEM(fields.shape, fields.dtype),
            pltpu.VMEM(bracket.shape, bracket.dtype),
            pltpu.VMEM(fraction.shape, fraction.dtype),
            pltpu.VMEM((var_count, row_count, plev_count, lons), jnp.bfloat16),
            dma((2,)),
            dma((var_count,)),
            dma((var_count,)),
            dma((lon_count,)),
            dma((lon_count,)),
            dma((lon_count,)),
            dma((lon_count,)),
            dma((2,)),
            dma((lon_count,)),
            dma((lon_count,)),
        ],
        compiler_params=pltpu.CompilerParams(
            collective_id=0, has_side_effects=True, vmem_limit_bytes=room + (8 << 20)
        ),
    )(*inputs)
    held = [pltpu.with_memory_space_constraint(x, pltpu.VMEM) for x in held]
    mean_shape = (var_count, own, plev_count)
    on_pressure, zonal_mean, meridional = pl.pallas_call(
        functools.partial(finish, lon_count, lat_count, float(lons * lon_count)),
        out_shape=(
            jax.ShapeDtypeStruct(rows_shape, jnp.bfloat16),
            jax.ShapeDtypeStruct(mean_shape, jnp.float32),
            jax.ShapeDtypeStruct(mean_shape, jnp.float32),
        ),
        in_specs=[in_vmem] * 4,
        out_specs=(anywhere,) * 3,
        scratch_shapes=[
            pltpu.VMEM(mean_shape, jnp.float32),
            pltpu.VMEM(mean_shape, jnp.float32),
            dma((3,)),
        ],
        compiler_params=pltpu.CompilerParams(vmem_limit_bytes=8 << 20),
    )(*held)
    return (
        on_pressure.transpose(0, 2, 1, 3),
        zonal_mean.transpose(0, 2, 1),
        meridional.transpose(0, 2, 1),
    )


def solution(mesh):
    return jax.shard_map(
        functools.partial(shards, mesh.shape["lon"], mesh.shape["lat"]),
        mesh=mesh,
        in_specs=(P(None, None, "lat", "lon"), P(None, "lat", "lon"), P(None, "lat", "lon")),
        out_specs=(
            P(None, None, ("lat", "lon"), None),
            P(None, None, ("lat", "lon")),
            P(None, None, ("lat", "lon")),
        ),
        check_vma=False,
    )
```
